32 devices in a mesh: groups: 2 (over x), seq: 8 (over z, y), head: 2 (over core).
Axes of the slice: x: 2, y: 2, z: 4, core: 2. Of those that a mesh axis runs over, the one named last changes fastest.
Arguments:
- queries: bfloat16 [2048, 6144], P(('groups', 'seq', 'head')), parts along dimension 0, may hold values from -600 to 600
- latents: bfloat16 [2048, 576], P(('groups', 'seq')), parts along dimension 0, may hold values from -600 to 600
- latent_gain: float32 [512], replicated, may hold values from 0.1 to 1.9
- key_up: bfloat16 [32, 128, 512], P('head'), may hold values from -0.5 to 0.5
- value_up: bfloat16 [32, 512, 128], P('head'), may hold values from -1 to 1
- out_weight: bfloat16 [4096, 7168], P('head', 'seq'), may hold values from -0.09375 to 0.09375
Outputs:
- mixed: bfloat16 [16, 2, 64, 7168], P('groups', 'head', None, 'seq'), parts along dimension 0
The draws below stay inside these ranges and needn't reach their ends.
There are 2 independent parts, one for each index of `groups`. The reference program is written for one: setup_inputs(seed, part) draws one part's arguments, and reference() takes and returns one part's arrays. A program takes and returns all parts, laid end to end along the dimension named above; an argument that names none is the same for every part. Nothing has to cross between parts.
All inputs are finite; a program needn't handle non-finite values.
Results may differ from the reference program's by a relative error of at most 0.013.
Values may be sent and summed in bfloat16 or wider, within the bound.
A program may use at most 128 MiB of HBM per device.

```python
import jax
import jax.numpy as jnp
from jax import lax

D = 7168
KV = 512
NOPE = 128
VD = 128
QK = 192
LATENT = 576
HEADS = 32
TOKENS = 1024
BLOCKS = 8
HSPLIT = 2
TOK_PIECE = 64


def draw_both(key):
    base_key = jax.random.fold_in(key, 7)
    keys = jax.random.split(base_key, 2)
    latent_vals = jnp.clip(jax.random.normal(keys[0], (TOKENS, LATENT), jnp.float32), -6.0, 6.0)
    query_vals = jnp.clip(jax.random.normal(keys[1], (TOKENS, HEADS * QK), jnp.float32), -6.0, 6.0)
    return (latent_vals, query_vals)


def draw_queries(key, part):
    return draw_both(key)[1].astype(jnp.bfloat16)


def draw_latents(key, part):
    return draw_both(key)[0].astype(jnp.bfloat16)


def block_levels(stream_key, shape, cuts, low, largest):
    gain = 1.0
    for dim, shards_of in cuts:
        draws = jax.random.uniform(jax.random.fold_in(jax.random.fold_in(stream_key, 6), dim), (shards_of,), jnp.float32, low / len(cuts), largest / len(cuts))
        gain = gain * jnp.repeat(jnp.exp(draws), shape[dim] // shards_of).reshape((-1,) + (1,) * (len(shape) - 1 - dim))
    return gain


def gaussian(rng, extent, deviation, limit, pieces=(), held_as=jnp.bfloat16):
    entries = deviation * jax.random.normal(rng, extent, jnp.float32)
    if pieces:
        entries = entries * block_levels(rng, extent, pieces, -0.22, 0.18)
    return jnp.clip(entries, -limit, limit).astype(held_as)


def setup_inputs(seed: int = 0, part: int = 0) -> dict:
    splits = jax.random.split(jax.random.key(seed), 7)
    part_splits = jax.random.split(jax.random.fold_in(splits[6], part), 7)
    queries = draw_queries(jax.random.fold_in(jax.random.fold_in(splits[6], part), 71), part)
    latents = draw_latents(jax.random.fold_in(jax.random.fold_in(splits[6], part), 71), part)
    latent_gain = jnp.clip(1.0 + 0.18 * jax.random.normal(splits[2], (KV,), jnp.float32), 0.1, 1.9)
    key_up = gaussian(splits[3], (HEADS, NOPE, KV), NOPE ** -0.5, 0.5, ((0, 2),))
    value_up = gaussian(splits[4], (HEADS, KV, VD), (KV // 16) ** -0.5, 1.0, ((0, 2),))
    out_weight = gaussian(splits[5], (HEADS * VD, D), (HEADS * VD) ** -0.5, 0.09375, ((0, 2), (1, 8)))
    return {"queries": queries, "latents": latents, "latent_gain": latent_gain, "key_up": key_up, "value_up": value_up, "out_weight": out_weight}


def rotate(values, position):
    middle = values.shape[-1] // 2
    frequency = 10000.0 ** (-jnp.arange(middle, dtype=jnp.float32) / middle)
    angles = position[..., None] * frequency
    former = values[..., :middle]
    latter = values[..., middle:]
    cosine = jnp.cos(angles)
    sin_part = jnp.sin(angles)
    return jnp.concatenate([former * cosine - latter * sin_part, former * sin_part + latter * cosine], -1)

def reference(queries, latents, latent_gain, key_up, value_up, out_weight):
    positions = jnp.arange(TOKENS).astype(jnp.float32)
    latent_f = latents.astype(jnp.float32)
    compressed = latent_f[:, :KV]
    spread = lax.optimization_barrier(jnp.mean(compressed * compressed, axis=-1, keepdims=True))
    normed = compressed * lax.rsqrt(spread + 1e-06) * latent_gain
    key_rope = rotate(latent_f[:, KV:], positions)
    key_rows = jnp.concatenate([normed, key_rope], -1).astype(jnp.bfloat16)
    query = queries.reshape(TOKENS, HEADS, QK)
    latent_query = jnp.einsum('thd,hdc->thc', query[..., :NOPE].astype(jnp.float32), key_up.astype(jnp.float32)).astype(jnp.bfloat16)
    rope_query = rotate(query[..., NOPE:].astype(jnp.float32), positions[:, None]).astype(jnp.bfloat16)
    query_rows = jnp.concatenate([latent_query, rope_query], -1)
    scale = QK ** (-0.5)
    visible = jnp.arange(TOKENS)[None, :] <= jnp.arange(TOKENS)[:, None]
    values = key_rows[:, :KV]

    def one_head(pair):
        head_query, head_value = pair
        scores = jnp.dot(head_query, key_rows.T, preferred_element_type=jnp.float32) * scale
        peak = lax.optimization_barrier(jnp.max(jnp.where(visible, scores, -1e+30), axis=-1))
        probs = jnp.where(visible, jnp.exp(scores - peak[:, None]), 0.0).astype(jnp.bfloat16)
        totals = lax.optimization_barrier(jnp.sum(probs.astype(jnp.float32), axis=-1))
        latent_out = (jnp.dot(probs, values, preferred_element_type=jnp.float32) / totals[:, None]).astype(jnp.bfloat16)
        return jnp.dot(latent_out, head_value, preferred_element_type=jnp.float32).astype(jnp.bfloat16)
    heads = lax.map(one_head, (jnp.transpose(query_rows, (1, 0, 2)), value_up))
    heads_out = jnp.transpose(heads, (1, 0, 2)).reshape(TOKENS, HEADS * VD)
    mixed = jnp.dot(heads_out, out_weight, preferred_element_type=jnp.float32).astype(jnp.bfloat16)
    return mixed.reshape(BLOCKS, HSPLIT, TOK_PIECE, D)
```

```python
import functools
import math

import jax
import jax.numpy as jnp
from jax import lax
from jax.experimental import pallas as pl
from jax.experimental.pallas import tpu as pltpu
from jax.sharding import PartitionSpec as P

MESH = pl.DeviceIdType.MESH
EPS = 1e-06
LANES = 128


def kernel(
    n,
    dims,
    q_hbm,
    lat_ref,
    gain_ref,
    tab_ref,
    kup_hbm,
    vup_hbm,
    w_hbm,
    out_ref,
    q_all,
    q_rows,
    keys,
    kup,
    vup,
    w,
    gath,
    part,
    own,
    sbuf,
    rbuf,
    local_sem,
    q_send,
    q_recv,
    k_send,
    k_recv,
    d_send,
    d_recv,
    r_send,
    r_recv,
    x_send,
    x_recv,
):
    heads, nope, rope, kv, vd, group = dims
    rows = lat_ref.shape[0]
    half_rows = rows // 2
    groups = heads // group
    total = n * rows
    slab = 2 * (nope + rope)
    width = keys.shape[-1]
    half_n = (n + 1) // 2
    gidx = lax.axis_index("groups")
    sidx = lax.axis_index("seq")
    h = lax.axis_index("head")
    odd = lax.rem(sidx, 2)
    place = (1 - odd) * (sidx // 2) + odd * (n - 1 - sidx // 2)

    def seq_of(position):
        position = lax.rem(position + 2 * n, n)
        upper = position // half_n
        return (1 - upper) * (2 * position) + upper * (2 * (n - 1 - position) + 1)

    partner = (gidx, sidx, 1 - h)

    half_cols = heads * (nope + rope)
    loads = [
        pltpu.make_async_copy(
            q_hbm.at[:, pl.ds(pl.multiple_of(h * half_cols, LANES), half_cols)],
            q_all.at[pl.ds(pl.multiple_of(h * half_rows, 16), half_rows)],
            local_sem.at[0],
        ),
        pltpu.make_async_copy(kup_hbm, kup, local_sem.at[1]),
        pltpu.make_async_copy(vup_hbm, vup, local_sem.at[2]),
        pltpu.make_async_copy(w_hbm, w, local_sem.at[3]),
    ]
    for load in loads:
        load.start()

    barrier = pltpu.get_barrier_semaphore()
    for other in ((gidx, seq_of(place + 1), h), (gidx, seq_of(place - 1), h), partner):
        pl.semaphore_signal(barrier, inc=1, device_id=other, device_id_type=MESH)

    latent = lat_ref[...].astype(jnp.float32)
    compressed = latent[:, :kv]
    spread = jnp.mean(compressed * compressed, axis=-1, keepdims=True)
    normed = compressed * lax.rsqrt(spread + EPS) * gain_ref[...]

    def rotate(raw):
        return (
            raw * tab_ref[0]
            + pltpu.roll(raw, LANES - rope // 2, 1) * tab_ref[1]
            + pltpu.roll(raw, rope // 2, 1) * tab_ref[2]
        )

    tail = jnp.concatenate(
        [latent[:, kv:], jnp.zeros((rows, LANES - rope), jnp.float32)], axis=1
    )
    keys[sidx, :, :kv] = normed.astype(jnp.bfloat16)
    keys[sidx, :, kv:] = rotate(tail).astype(jnp.bfloat16)

    pl.semaphore_wait(barrier, 3)

    q_copy = pltpu.make_async_remote_copy(
        src_ref=q_hbm.at[:, pl.ds(pl.multiple_of((1 - h) * half_cols, LANES), half_cols)],
        dst_ref=q_all.at[pl.ds(pl.multiple_of(h * half_rows, 16), half_rows)],
        send_sem=q_send,
        recv_sem=q_recv,
        device_id=partner,
        device_id_type=MESH,
    )

    def key_hop(way, step):
        sign = 1 - 2 * way
        piece = keys.at[
            seq_of(place - sign * step), pl.ds(pl.multiple_of(h * half_rows, 16), half_rows)
        ]
        return pltpu.make_async_remote_copy(
            src_ref=piece,
            dst_ref=piece,
            send_sem=k_send.at[way, step],
            recv_sem=k_recv.at[way, step],
            device_id=(gidx, seq_of(place + sign), h),
            device_id_type=MESH,
        )

    def key_pass(way, step, side):
        sign = 1 - 2 * way
        piece = keys.at[
            seq_of(place - sign * (step + 1)),
            pl.ds(pl.multiple_of(side * half_rows, 16), half_rows),
        ]
        return pltpu.make_async_remote_copy(
            src_ref=piece,
            dst_ref=piece,
            send_sem=d_send.at[way, step],
            recv_sem=d_recv.at[way, step],
            device_id=partner,
            device_id_type=MESH,
        )

    hops = (n // 2, n - 1 - n // 2)
    for way in range(2):
        if hops[way] > 0:
            key_hop(way, 0).start()
    q_copy.start()
    loads[0].wait()
    loads[1].wait()

    def lift(pair):
        start = pl.multiple_of(pair * slab, LANES)
        first = q_all[:, pl.ds(start, nope)]
        second = q_all[:, pl.ds(pl.multiple_of(start + nope, LANES), slab - nope)].astype(
            jnp.float32
        )
        moved = pltpu.roll(second, slab - nope - rope, 1)
        raws = (second[:, :LANES], moved[:, nope : nope + LANES])
        flat = (first, moved[:, :nope].astype(jnp.bfloat16))
        for i in range(2):
            head = 2 * pair + i
            q_rows[head, :, :kv] = jnp.dot(
                flat[i], kup[head], preferred_element_type=jnp.float32
            ).astype(jnp.bfloat16)
            q_rows[head, :, kv:] = rotate(raws[i]).astype(jnp.bfloat16)

    def key_step(step):
        for way in range(2):
            if step <= hops[way]:
                key_hop(way, step - 1).wait_recv()
                if step < hops[way]:
                    key_hop(way, step).start()
                key_pass(way, step - 1, h).start()

    pairs = heads // 2
    per_step = -(-pairs // max(hops[0], 1))
    done = 0
    q_copy.wait_recv()
    for step in range(1, hops[0] + 1):
        count = min(per_step, pairs - done)
        if count > 0:

            def some(i, carry):
                lift(i)
                return carry

            lax.fori_loop(done, done + count, some, 0)
            done += count
        key_step(step)
    for way in range(2):
        for step in range(hops[way]):
            key_pass(way, step, h).wait_recv()
    loads[2].wait()

    def ring_hop(chunk, step):
        sign = 1 - 2 * lax.rem(chunk, 2)
        piece = gath.at[seq_of(place - sign * step), chunk]
        return pltpu.make_async_remote_copy(
            src_ref=piece,
            dst_ref=piece,
            send_sem=r_send.at[chunk, step],
            recv_sem=r_recv.at[chunk, step],
            device_id=(gidx, seq_of(place + sign), h),
            device_id_type=MESH,
        )

    factor = (nope + rope) ** (-0.5) * math.log2(math.e)

    def attend(g, carry):
        query = q_rows[pl.ds(g * group, group)].reshape(group * rows, width)
        all_keys = keys[...].reshape(total, width)
        scores = lax.dot_general(
            query, all_keys, (((1,), (1,)), ((), ())), preferred_element_type=jnp.float32
        )
        column = lax.broadcasted_iota(jnp.int32, (rows, total), 1)
        line = lax.broadcasted_iota(jnp.int32, (rows, total), 0) + sidx * rows
        visible = column <= line
        scores = jnp.where(visible[None], scores.reshape(group, rows, total), -1e30)
        peak = jnp.max(scores, axis=-1, keepdims=True)
        probs = jnp.exp2((scores - peak) * factor).astype(jnp.bfloat16)
        sums = jnp.sum(probs.astype(jnp.float32), axis=-1, keepdims=True)
        mixed = jnp.dot(
            probs.reshape(group * rows, total),
            all_keys[:, :kv],
            preferred_element_type=jnp.float32,
        ).reshape(group, rows, kv)
        latent_out = (mixed / sums).astype(jnp.bfloat16)
        for i in range(group):
            gath[sidx, g, :, i * vd : (i + 1) * vd] = jnp.dot(
                latent_out[i], vup[g * group + i], preferred_element_type=jnp.float32
            ).astype(jnp.bfloat16)
        ring_hop(g, 0).start()

        @pl.when(g >= 2)
        def _():
            ring_hop(g - 2, 0).wait_recv()
            ring_hop(g - 2, 1).start()

        return carry

    lax.fori_loop(0, groups, attend, 0)
    loads[3].wait()

    def exchange(block):
        return pltpu.make_async_remote_copy(
            src_ref=sbuf.at[block],
            dst_ref=rbuf.at[block],
            send_sem=x_send.at[block],
            recv_sem=x_recv.at[block],
            device_id=partner,
            device_id_type=MESH,
        )

    def finish(block):
        value = None
        for c in range(groups):
            term = jnp.dot(gath[block, c], w[c], preferred_element_type=jnp.float32)
            value = term if value is None else value + term
        part[...] = value.reshape(part.shape)
        sbuf[block] = part[1 - h].astype(jnp.bfloat16)
        own[block] = part[h]
        exchange(block).start()

    for c in range(max(groups - 2, 0), groups):
        ring_hop(c, 0).wait_recv()
        ring_hop(c, 1).start()
    finish(sidx)

    def ring_step(step, carry):
        for c in range(groups):
            ring_hop(c, step - 1).wait_recv()

            @pl.when(step < n - 1)
            def _():
                ring_hop(c, step).start()

        @pl.when(2 * step >= n)
        def _():
            finish(seq_of(place - step))

        @pl.when(2 * step > n)
        def _():
            finish(seq_of(place + step))

        return carry

    lax.fori_loop(2, n, ring_step, 0)

    def close(step, carry):
        block = seq_of(place + step)
        exchange(block).wait_recv()
        out_ref[block] = (own[block] + rbuf[block].astype(jnp.float32)).astype(out_ref.dtype)
        exchange(block).wait_send()
        return carry

    lax.fori_loop(0, n, close, 0)

    q_copy.wait_send()
    for way in range(2):
        for step in range(hops[way]):
            key_hop(way, step).wait_send()
            key_pass(way, step, h).wait_send()

    def drain(step, carry):
        for c in range(groups):
            ring_hop(c, step).wait_send()
        return carry

    lax.fori_loop(0, n - 1, drain, 0)


def local(queries, latents, latent_gain, key_up, value_up, out_weight):
    n = lax.axis_size("seq")
    seq_index = lax.axis_index("seq")
    heads, nope, kv = key_up.shape
    vd = value_up.shape[-1]
    rope = latents.shape[-1] - kv
    rows = latents.shape[0]
    columns = out_weight.shape[-1]
    group = 4 if heads % 8 == 0 and n * rows <= 2048 else 2
    chunks = heads // group
    width = kv + LANES
    half = rope // 2
    frequency = 10000.0 ** (-jnp.arange(half, dtype=jnp.float32) / half)
    position = (seq_index * rows + jnp.arange(rows)).astype(jnp.float32)
    angles = position[:, None] * frequency
    cosine, sine = jnp.cos(angles), jnp.sin(angles)
    zero = jnp.zeros_like(sine)
    fill = jnp.zeros((rows, LANES - rope), jnp.float32)
    table = jnp.stack(
        [
            jnp.concatenate([cosine, cosine, fill], -1),
            jnp.concatenate([-sine, zero, fill], -1),
            jnp.concatenate([zero, sine, fill], -1),
        ]
    )
    bf16, f32 = jnp.bfloat16, jnp.float32
    dma = pltpu.SemaphoreType.DMA
    hops = max(n // 2, 1)
    any_spec = pl.BlockSpec(memory_space=pl.ANY)
    vmem_spec = pl.BlockSpec(memory_space=pltpu.VMEM)
    out = pl.pallas_call(
        functools.partial(kernel, n, (heads, nope, rope, kv, vd, group)),
        out_shape=jax.ShapeDtypeStruct((n, rows // 2, columns), bf16),
        in_specs=[any_spec, vmem_spec, vmem_spec, vmem_spec, any_spec, any_spec, any_spec],
        out_specs=vmem_spec,
        scratch_shapes=[
            pltpu.VMEM((rows, heads * (nope + rope)), bf16),
            pltpu.VMEM((heads, rows, width), bf16),
            pltpu.VMEM((n, rows, width), bf16),
            pltpu.VMEM(key_up.shape, bf16),
            pltpu.VMEM(value_up.shape, bf16),
            pltpu.VMEM((chunks, group * vd, columns), bf16),
            pltpu.VMEM((n, chunks, rows, group * vd), bf16),
            pltpu.VMEM((2, rows // 2, columns), f32),
            pltpu.VMEM((n, rows // 2, columns), f32),
            pltpu.VMEM((n, rows // 2, columns), bf16),
            pltpu.VMEM((n, rows // 2, columns), bf16),
            dma((4,)),
            dma,
            dma,
            dma((2, hops)),
            dma((2, hops)),
            dma((2, hops)),
            dma((2, hops)),
            dma((chunks, n - 1)),
            dma((chunks, n - 1)),
            dma((n,)),
            dma((n,)),
        ],
        compiler_params=pltpu.CompilerParams(
            collective_id=0, has_side_effects=True, vmem_limit_bytes=66 * 1000 * 1000
        ),
        name="layer",
    )(
        queries,
        latents,
        latent_gain.reshape(1, kv),
        table,
        key_up,
        value_up,
        out_weight.reshape(chunks, group * vd, columns),
    )
    return out.reshape(n, 1, rows // 2, columns)


def solution(mesh):
    placed = (
        P(("groups", "seq", "head"), None),
        P(("groups", "seq"), None),
        P(),
        P("head", None, None),
        P("head", None, None),
        P("head", "seq"),
    )
    return jax.shard_map(
        local,
        mesh=mesh,
        in_specs=placed,
        out_specs=P("groups", "head", None, "seq"),
        check_vma=False,
    )
```
